32 devices in a mesh: dp: 2 (over x), seq: 16 (over z, y, core).
Axes of the slice: x: 2, y: 2, z: 4, core: 2. Of those that a mesh axis runs over, the one named last changes fastest.
Arguments:
- tiles: bfloat16 [2, 16, 32, 4, 1024], P('dp', None, 'seq'), may hold values from -6 to 6
- patch_index: int32 [2, 16, 32, 4], P('dp', None, 'seq'), may hold values from 0 to 127
- pos_table: bfloat16 [128, 1024], replicated, may hold values from -6 to 6
- depth_kernel: bfloat16 [2, 27, 1024], replicated, may hold values from -1.25 to 1.25
- enc_gain: bfloat16 [2, 1024], replicated, may hold values from 0.099609375 to 1.8984375
- point_weight: bfloat16 [2, 1024, 1024], replicated, may hold values from -0.1875 to 0.1875
- action_ids: int32 [2, 16], replicated, may hold values from 0 to 7
- w_in: bfloat16 [1024, 5120], P('seq', 'dp'), may hold values from -0.1875 to 0.1875
- action_table: bfloat16 [8, 5120], P(None, 'dp'), may hold values from -6 to 6
- dyn_gain: bfloat16 [5120], P('dp'), may hold values from 0.099609375 to 1.8984375
- w_query: bfloat16 [5120, 5120], P('seq', 'dp'), may hold values from -0.078125 to 0.078125
- w_keyval: bfloat16 [5120, 2, 1024], P('seq', None, 'dp'), may hold values from -0.078125 to 0.078125
- seq_order: int32 [4], replicated, may hold values from 0 to 3, each once
Outputs:
- attended: bfloat16 [2, 16, 32, 4, 5120], P(None, None, 'seq', None, 'dp')
The draws below stay inside these ranges and needn't reach their ends.
Inputs may be any that keep to these rules, and one draw needn't show every extreme that they name: `seq_order`: each of 0 to 3 appears once.
All inputs are finite; a program needn't handle non-finite values.
Results may differ from the reference program's by a relative error of at most 0.012.
Values may be sent and summed in bfloat16 or wider, within the bound.
A program may use at most 128 MiB of HBM per device.

```python
import jax
import jax.numpy as jnp
from jax import lax

ENC = 1024
DIM = 5120
HEAD = 128
Q_HEADS = 40
KV_HEADS = 8
ACTIONS = 8
FRAMES = 16
LAYERS = 2
COLS = 4
CLIPS = 2
ROWS = 32
POSITIONS = 128


def with_ends(values, key, low, top_value):
    dims = values.shape
    spot = [jax.random.randint(jax.random.fold_in(key, axis), (), 0, dims[axis]) for axis in range(len(dims))]
    values = values.at[tuple(spot)].set(low)
    longest = dims.index(max(dims))
    spot[longest] = (spot[longest] + 1) % dims[longest]
    return values.at[tuple(spot)].set(top_value)


def steps_of(stream_key, shape, split, least, high):
    factor_of, own = 1.0, jax.random.fold_in(stream_key, 6)
    for dim, blocks in split:
        draws = jnp.exp(jax.random.uniform(jax.random.fold_in(own, dim), (blocks,), jnp.float32, least / len(split), high / len(split)))
        factor_of = factor_of * jnp.repeat(draws, shape[dim] // blocks).reshape([-1 if axis == dim else 1 for axis in range(len(shape))])
    return factor_of


def scatter_about(stream_key, dims, width, limit, shards=(), kind=jnp.bfloat16):
    entries = width * jax.random.normal(stream_key, dims, jnp.float32)
    if shards:
        entries = entries * steps_of(stream_key, dims, shards, -0.22, 0.18)
    return jnp.clip(entries, -limit, limit).astype(kind)


def setup_inputs(seed: int = 0) -> dict:
    arg_keys = jax.random.split(jax.random.key(seed), 14)
    return {
        "tiles": scatter_about(arg_keys[0], (CLIPS, FRAMES, ROWS, COLS, ENC), 1.0, 6.0, ((0, 2), (2, 16))),
        "patch_index": with_ends(jax.random.randint(arg_keys[1], (CLIPS, FRAMES, ROWS, COLS), 0, POSITIONS), jax.random.fold_in(arg_keys[1], 1), 0, POSITIONS - 1).astype(jnp.int32),
        "pos_table": scatter_about(arg_keys[2], (POSITIONS, ENC), 1.0, 6.0),
        "depth_kernel": scatter_about(arg_keys[3], (LAYERS, 27, ENC), 27 ** -0.5, 1.25),
        "enc_gain": jnp.clip(1.0 + 0.18 * jax.random.normal(arg_keys[4], (LAYERS, ENC), jnp.float32), 0.099609375, 1.8984375).astype(jnp.bfloat16),
        "point_weight": scatter_about(arg_keys[5], (LAYERS, ENC, ENC), ENC ** -0.5, 0.1875),
        "action_ids": with_ends(jax.random.randint(arg_keys[6], (CLIPS, FRAMES), 0, ACTIONS), jax.random.fold_in(arg_keys[6], 1), 0, ACTIONS - 1).astype(jnp.int32),
        "w_in": scatter_about(arg_keys[7], (ENC, DIM), ENC ** -0.5, 0.1875, ((0, 16), (1, 2))),
        "action_table": scatter_about(arg_keys[8], (ACTIONS, DIM), 1.0, 6.0, ((1, 2),)),
        "dyn_gain": jnp.clip(1.0 + 0.18 * jax.random.normal(arg_keys[9], (DIM,), jnp.float32), 0.099609375, 1.8984375).astype(jnp.bfloat16),
        "w_query": scatter_about(arg_keys[10], (DIM, DIM), DIM ** -0.5, 0.078125, ((0, 16), (1, 2))),
        "w_keyval": scatter_about(arg_keys[11], (DIM, 2, KV_HEADS * HEAD), DIM ** -0.5, 0.078125, ((0, 16), (2, 2))),
        "seq_order": jax.random.permutation(arg_keys[12], COLS).astype(jnp.int32),
    }


def depth_block(padded, kernel, gains, weight):
    frames = padded.shape[1]
    height = padded.shape[2] - 2
    breadth = padded.shape[3]
    channels = padded.shape[4]
    framed = jnp.pad(padded.astype(jnp.float32), ((0, 0), (2, 0), (0, 0), (1, 1), (0, 0)))
    summed = jnp.zeros((padded.shape[0], frames, height, breadth, channels), jnp.float32)
    for time_tap in range(3):
        for row_tap in range(3):
            for col_tap in range(3):
                window = framed[:, time_tap:time_tap + frames, row_tap:row_tap + height, col_tap:col_tap + breadth, :]
                summed = summed + window * kernel[9 * time_tap + 3 * row_tap + col_tap].astype(jnp.float32)
    factor = lax.rsqrt(lax.optimization_barrier(jnp.mean(summed * summed, axis=-1, keepdims=True)) + 1e-05)
    normed = (summed * factor * gains.astype(jnp.float32)).astype(jnp.bfloat16)
    projected = jnp.dot(normed.reshape(-1, channels), weight, preferred_element_type=jnp.float32).reshape(summed.shape)
    centre = padded[:, :, 1:-1].astype(jnp.float32)
    return (centre + jax.nn.gelu(projected)).astype(jnp.bfloat16)

def temporal_mix(query_heads, key_heads, value_heads):
    frames = query_heads.shape[1]
    query_unit = query_heads * lax.rsqrt(lax.optimization_barrier(jnp.mean(query_heads * query_heads, axis=-1, keepdims=True)) + 1e-06)
    key_unit = key_heads * lax.rsqrt(lax.optimization_barrier(jnp.mean(key_heads * key_heads, axis=-1, keepdims=True)) + 1e-06)
    scores = jnp.einsum('cfpkgh,ctpkh->cpkgft', query_unit, key_unit, precision=lax.Precision.HIGHEST) * HEAD ** (-0.5)
    causal = jnp.arange(frames, dtype=jnp.int32)[:, None] >= jnp.arange(frames, dtype=jnp.int32)[None, :]
    raised = jnp.where(causal, jnp.exp(scores), 0.0)
    shares = (raised / lax.optimization_barrier(jnp.sum(raised, axis=-1, keepdims=True))).astype(jnp.bfloat16)
    mixed = jnp.einsum('cpkgft,ctpkh->cfpkgh', shares.astype(jnp.float32), value_heads.astype(jnp.float32), precision=lax.Precision.HIGHEST)
    return mixed.astype(jnp.bfloat16)

def reference(tiles, patch_index, pos_table, depth_kernel, enc_gain, point_weight, action_ids, w_in, action_table, dyn_gain, w_query, w_keyval, seq_order):
    placed = jnp.take(pos_table, patch_index, axis=0).astype(jnp.float32)
    hidden = (tiles.astype(jnp.float32) + placed).astype(jnp.bfloat16)
    for block_idx in range(LAYERS):
        padded = jnp.pad(hidden, ((0, 0), (0, 0), (1, 1), (0, 0), (0, 0)))
        hidden = depth_block(padded, depth_kernel[block_idx], enc_gain[block_idx], point_weight[block_idx])
    group = Q_HEADS // KV_HEADS
    cells = ROWS * COLS

    def one_clip(inputs_pair):
        latent, frame_ids = inputs_pair
        embed = jnp.dot(latent.reshape(-1, ENC), w_in, preferred_element_type=jnp.float32).reshape(FRAMES, cells, DIM)
        embed = embed + jnp.take(action_table, frame_ids, axis=0).astype(jnp.float32)[:, None, :]
        embed = jax.nn.gelu(embed)
        factor = lax.rsqrt(lax.optimization_barrier(jnp.mean(embed * embed, axis=-1, keepdims=True)) + 1e-05)
        normed = (embed * factor * dyn_gain.astype(jnp.float32)).astype(jnp.bfloat16).reshape(-1, DIM)
        query = jnp.dot(normed, w_query, preferred_element_type=jnp.float32)
        keyval = jnp.dot(normed, w_keyval.reshape(DIM, -1), preferred_element_type=jnp.float32)
        query_heads = query.reshape(1, FRAMES, cells, KV_HEADS, group, HEAD)
        pairs = keyval.reshape(1, FRAMES, cells, 2, KV_HEADS, HEAD)
        mixed = temporal_mix(query_heads, pairs[:, :, :, 0], pairs[:, :, :, 1].astype(jnp.bfloat16))
        return mixed.reshape(FRAMES, ROWS, COLS, DIM)
    mixed_all = lax.map(one_clip, (hidden, action_ids))
    return jnp.take(mixed_all, seq_order, axis=3)
```

```python
import functools
import math

import jax
import jax.numpy as jnp
from jax import lax
from jax.experimental import pallas as pl
from jax.experimental.pallas import tpu as pltpu
from jax.sharding import PartitionSpec as P

DIM = 5120
HEAD = 128
Q_HEADS = 40
KV_HEADS = 8
MESH = pl.DeviceIdType.MESH


def extended(block, sides, width):
    for axis, dim in sides:
        count = lax.axis_size(axis)
        forward = [(i, i + 1) for i in range(count - 1)]
        backward = [(target, source) for source, target in forward]
        low = lax.ppermute(
            lax.slice_in_dim(block, block.shape[dim] - width, None, axis=dim), axis, forward
        )
        high = lax.ppermute(lax.slice_in_dim(block, 0, width, axis=dim), axis, backward)
        block = jnp.concatenate([low, block, high], axis=dim)
    return block


def depth_block(padded, kernel, gains, weight):
    frames = padded.shape[1]
    height = padded.shape[2] - 2
    breadth = padded.shape[3]
    channels = padded.shape[4]
    framed = jnp.pad(padded.astype(jnp.float32), ((0, 0), (2, 0), (0, 0), (1, 1), (0, 0)))
    summed = jnp.zeros((padded.shape[0], frames, height, breadth, channels), jnp.float32)
    for time_tap in range(3):
        for row_tap in range(3):
            for col_tap in range(3):
                window = framed[
                    :,
                    time_tap : time_tap + frames,
                    row_tap : row_tap + height,
                    col_tap : col_tap + breadth,
                    :,
                ]
                summed = summed + window * kernel[9 * time_tap + 3 * row_tap + col_tap].astype(
                    jnp.float32
                )
    factor = lax.rsqrt(jnp.mean(summed * summed, axis=-1, keepdims=True) + 1e-05)
    normed = (summed * factor * gains.astype(jnp.float32)).astype(jnp.bfloat16)
    projected = jnp.dot(
        normed.reshape(-1, channels), weight, preferred_element_type=jnp.float32
    ).reshape(summed.shape)
    centre = padded[:, :, 1:-1].astype(jnp.float32)
    return (centre + jax.nn.gelu(projected)).astype(jnp.bfloat16)


def gelu(z):
    return 0.5 * z * (1.0 + jnp.tanh(0.7978845608028654 * (z + 0.044715 * (z * z * z))))


def flipped(t, mask, bits):
    for bit in bits:
        if mask & bit:
            t = t + bit - 2 * bit * ((t // bit) % 2)
    return t


def window_kernel(
    sizes,
    pack_ref,
    in_ref,
    aux_ref,
    latent_ref,
    pick_ref,
    out_ref,
    w_all,
    in_all,
    aux_all,
    lat_all,
    embeds,
    squares,
    mixed,
    w_send,
    w_recv,
    i_send,
    i_recv,
    l_send,
    l_recv,
    a_send,
    a_recv,
    o_send,
    o_recv,
    own_sem,
):
    D, C, T, cells, kvg = sizes
    d = lax.axis_index("dp")
    seq = lax.axis_index("seq")
    c = seq // T
    t = seq % T
    bits = []
    bit = T // 2
    while bit:
        bits.append(bit)
        bit //= 2
    depth = pack_ref.shape[1]
    in_rows, in_cols = in_ref.shape
    tokens = latent_ref.shape[0]
    group = Q_HEADS // KV_HEADS
    qcols = kvg * group * HEAD

    def to_c(shift):
        return (d, ((c + shift) % C) * T + t)

    def to_t(bit):
        return (d, c * T + flipped(t, bit, bits))

    def to_d(shift):
        return ((d + shift) % D, seq)

    peers = [to_c(s) for s in range(1, C)] + [to_t(b) for b in bits] + [to_d(s) for s in range(1, D)]
    barrier = pltpu.get_barrier_semaphore()
    for peer in peers:
        pl.semaphore_signal(barrier, inc=1, device_id=peer, device_id_type=MESH)
    pl.semaphore_wait(barrier, len(peers))

    sends = []

    def push(src, dst, send_sem, recv_sem, peer):
        copy = pltpu.make_async_remote_copy(
            src_ref=src,
            dst_ref=dst,
            send_sem=send_sem,
            recv_sem=recv_sem,
            device_id=peer,
            device_id_type=MESH,
        )
        copy.start()
        sends.append(copy)

    def arrived(ref, sem):
        pltpu.make_async_copy(ref, ref, sem).wait()

    def w_slot(s, m):
        origin = ((c + C - s) % C) * T + flipped(t, m, bits)
        return w_all.at[pl.ds(pl.multiple_of(origin * depth, depth), depth)]

    def i_slot(s, m, e):
        origin = ((c + C - s) % C) * T + flipped(t, m, bits)
        column = ((d + D - e) % D) * in_cols
        return in_all.at[
            pl.ds(pl.multiple_of(origin * in_rows, in_rows), in_rows),
            pl.ds(pl.multiple_of(column, HEAD), in_cols),
        ]

    def l_slot(s, e):
        row = ((d + D - e) % D) * tokens
        return lat_all.at[(c + C - s) % C, pl.ds(pl.multiple_of(row, tokens), tokens)]

    def a_slot(e):
        column = ((d + D - e) % D) * in_cols
        return aux_all.at[:, pl.ds(pl.multiple_of(column, HEAD), in_cols)]

    def w_forward(s, m, src):
        low = -1
        for b in bits:
            if m & b:
                low = bits.index(b)
        for index in range(low + 1, len(bits)):
            b = bits[index]
            push(src, w_slot(s, m), w_send.at[s, m | b], w_recv.at[s, m | b], to_t(b))

    early, last = bits[:-1], bits[-1]

    def i_forward(s, m, e, src):
        low = -1
        for b in early:
            if m & b:
                low = bits.index(b)
        if e == 0:
            for index in range(low + 1, len(early)):
                b = early[index]
                push(src, i_slot(s, m, e), i_send.at[s, m | b, e], i_recv.at[s, m | b, e], to_t(b))
            for shift in range(1, D):
                push(src, i_slot(s, m, e), i_send.at[s, m, shift], i_recv.at[s, m, shift], to_d(shift))
        push(src, i_slot(s, m, e), i_send.at[s, m | last, e], i_recv.at[s, m | last, e], to_t(last))

    def l_forward(s, src):
        for e in range(1, D):
            push(src, l_slot(s, 0), l_send.at[s, e], l_recv.at[s, e], to_d(e))

    own = [
        pltpu.make_async_copy(pack_ref.at[c], w_slot(0, 0), own_sem.at[0]),
        pltpu.make_async_copy(in_ref, i_slot(0, 0, 0), own_sem.at[1]),
        pltpu.make_async_copy(latent_ref, l_slot(0, 0), own_sem.at[2]),
        pltpu.make_async_copy(aux_ref, a_slot(0), own_sem.at[3]),
    ]
    for copy in own:
        copy.start()
    for shift in range(1, D):
        push(aux_ref, a_slot(0), a_send.at[shift], a_recv.at[shift], to_d(shift))
    for shift in range(1, C):
        push(in_ref, i_slot(0, 0, 0), i_send.at[shift, 0, 0], i_recv.at[shift, 0, 0], to_c(shift))
    i_forward(0, 0, 0, in_ref)
    for shift in range(1, C):
        push(latent_ref, l_slot(0, 0), l_send.at[shift, 0], l_recv.at[shift, 0], to_c(shift))
    l_forward(0, latent_ref)
    for shift in range(1, C):
        push(
            pack_ref.at[(c + shift) % C],
            w_slot(0, 0),
            w_send.at[shift, 0],
            w_recv.at[shift, 0],
            to_c(shift),
        )
    w_forward(0, 0, pack_ref.at[c])

    def i_event(s, m, e):
        arrived(i_slot(s, m, e), i_recv.at[s, m, e])
        if not m & last:
            i_forward(s, m, e, i_slot(s, m, e))

    def w_event(s, m):
        arrived(w_slot(s, m), w_recv.at[s, m])
        w_forward(s, m, w_slot(s, m))

    def l_event(s, e):
        arrived(l_slot(s, e), l_recv.at[s, e])
        if e == 0:
            l_forward(s, l_slot(s, e))

    order_w = sorted(
        ((m.bit_count(), s, m) for s in range(C) for m in range(T) if s or m),
        key=lambda item: (item[0] + item[1], item[0]),
    )
    w_todo = [(s, m) for _, s, m in order_w]
    for s in range(1, C):
        i_event(s, 0, 0)
    for m in sorted((m for m in range(1, T) if not m & last), key=lambda m: m.bit_count()):
        for s in range(C):
            i_event(s, m, 0)
    for s in range(1, C):
        l_event(s, 0)
    for e in range(1, D):
        arrived(a_slot(e), a_recv.at[e])
        for m in range(T):
            if not m & last:
                for s in range(C):
                    i_event(s, m, e)
    for s, m in list(w_todo):
        if m == 0:
            w_event(s, m)
            w_todo.remove((s, m))
    for m in range(T):
        if m & last:
            for e in range(D):
                for s in range(C):
                    i_event(s, m, e)
    for e in range(1, D):
        for s in range(C):
            l_event(s, e)
    for copy in own:
        copy.wait()

    chunk = 512
    rows = D * tokens

    def embed_block(shift):
        where = (c + shift) % C
        squares[where] = jnp.zeros((rows, HEAD), jnp.float32)

        def step(j, carry):
            cols = pl.ds(pl.multiple_of(j * chunk, chunk), chunk)
            z = jnp.dot(lat_all[where], in_all[:, cols], preferred_element_type=jnp.float32)
            z = z + jnp.dot(pick_ref[...], aux_all[:, cols], preferred_element_type=jnp.float32)
            g = gelu(z)
            gain = aux_all[:, cols].astype(jnp.float32)[8:9]
            embeds[where, :, cols] = (g * gain).astype(jnp.bfloat16)
            square = g * g
            part = square[:, :HEAD]
            for k in range(1, chunk // HEAD):
                part = part + square[:, k * HEAD : (k + 1) * HEAD]
            squares[where] += part
            return carry

        lax.fori_loop(0, embeds.shape[2] // chunk, step, 0)

    per = -(-len(w_todo) // C)
    for shift in range(C):
        embed_block(shift)
        for s, m in w_todo[shift * per : (shift + 1) * per]:
            w_event(s, m)

    row_ids = lax.broadcasted_iota(jnp.int32, (tokens, tokens), 0)
    col_ids = lax.broadcasted_iota(jnp.int32, (tokens, tokens), 1)
    seen = (row_ids % cells == col_ids % cells) & (row_ids // cells >= col_ids // cells)

    def unit(x):
        return x * lax.rsqrt(jnp.mean(x * x, axis=-1, keepdims=True) + 1e-06)

    def mix_block(where):
        total = jnp.dot(embeds[where], w_all[...], preferred_element_type=jnp.float32)
        mean = jnp.sum(squares[where], axis=-1, keepdims=True) / DIM
        total = total * lax.rsqrt(mean + 1e-05)
        for kv in range(kvg):
            at = qcols + kv * HEAD
            key = unit(total[:, at : at + HEAD]).astype(jnp.bfloat16)
            at = qcols + (kvg + kv) * HEAD
            value = total[:, at : at + HEAD].astype(jnp.bfloat16)
            for h in range(kv * group, (kv + 1) * group):
                query = unit(total[:, h * HEAD : (h + 1) * HEAD]) * HEAD**-0.5
                query = query.astype(jnp.bfloat16)
                for clip in range(D):
                    span = slice(clip * tokens, (clip + 1) * tokens)
                    score = lax.dot_general(
                        query[span],
                        key[span],
                        (((1,), (1,)), ((), ())),
                        preferred_element_type=jnp.float32,
                    )
                    raised = jnp.where(seen, jnp.exp(score), 0.0)
                    shares = raised / jnp.sum(raised, axis=-1, keepdims=True)
                    result = jnp.dot(
                        shares.astype(jnp.bfloat16), value[span], preferred_element_type=jnp.float32
                    )
                    mixed[where, span, h * HEAD : (h + 1) * HEAD] = result.astype(jnp.bfloat16)

    mine = pl.ds(pl.multiple_of(c * qcols, HEAD), qcols)

    def send_of(shift):
        where = (c + shift) % C
        return pltpu.make_async_remote_copy(
            src_ref=mixed.at[where],
            dst_ref=out_ref.at[:, mine],
            send_sem=o_send.at[shift],
            recv_sem=o_recv.at[shift],
            device_id=(d, where * T + t),
            device_id_type=MESH,
        )

    def mix_step(index, carry):
        shift = index + 1
        mix_block((c + shift) % C)
        send_of(shift).start()
        return carry

    lax.fori_loop(0, C - 1, mix_step, 0)
    mix_block(c)
    keep = pltpu.make_async_copy(mixed.at[c], out_ref.at[:, mine], own_sem.at[0])
    keep.start()
    for shift in range(1, C):
        send_of(shift).wait_send()
        column = ((c + C - shift) % C) * qcols
        arrived(out_ref.at[:, pl.ds(pl.multiple_of(column, HEAD), qcols)], o_recv.at[shift])
    keep.wait()
    for copy in sends:
        copy.wait_send()


def body(
    tiles,
    patch_index,
    pos_table,
    depth_kernel,
    enc_gain,
    point_weight,
    action_ids,
    w_in,
    action_table,
    dyn_gain,
    w_query,
    w_keyval,
    seq_order,
):
    clip_local, frames, height, breadth, channels = tiles.shape
    positions = pos_table.shape[0]
    blocks = depth_kernel.shape[0]
    D, S = lax.axis_size("dp"), lax.axis_size("seq")
    kv_local = w_keyval.shape[2] // HEAD
    C = math.gcd(kv_local, S)
    T = S // C
    assert T & (T - 1) == 0 and T > 1 and clip_local == 1
    kvg = kv_local // C
    group = Q_HEADS // KV_HEADS
    depth = w_query.shape[0]

    flat_index = patch_index.reshape(-1)
    position_pick = (flat_index[:, None] == jnp.arange(positions, dtype=jnp.int32)[None, :]).astype(
        jnp.bfloat16
    )
    placed = jnp.dot(position_pick, pos_table, preferred_element_type=jnp.float32).reshape(
        tiles.shape
    )
    hidden = (tiles.astype(jnp.float32) + placed).astype(jnp.bfloat16)
    for block_idx in range(blocks):
        padded = extended(hidden, (("seq", 2),), 1)
        hidden = depth_block(
            padded, depth_kernel[block_idx], enc_gain[block_idx], point_weight[block_idx]
        )
    latent = jnp.take(hidden, seq_order, axis=3).reshape(-1, channels)

    cells = height * breadth
    tokens = frames * cells
    pack = jnp.concatenate(
        [
            w_query.reshape(depth, C, -1).transpose(1, 0, 2),
            w_keyval.reshape(depth, 2, C, -1).transpose(2, 0, 1, 3).reshape(C, depth, -1),
        ],
        axis=2,
    )
    actions = action_table.shape[0]
    assert actions == 8
    aux = jnp.concatenate(
        [action_table, dyn_gain[None], jnp.zeros((7, action_table.shape[1]), jnp.bfloat16)], axis=0
    )
    pick = (
        jnp.repeat(action_ids.reshape(-1), cells)[:, None] == jnp.arange(16, dtype=jnp.int32)[None]
    ).astype(jnp.bfloat16)
    width = pack.shape[2]
    qcols = kvg * group * HEAD
    bf16, f32 = jnp.bfloat16, jnp.float32
    dma = pltpu.SemaphoreType.DMA
    out = pl.pallas_call(
        functools.partial(window_kernel, (D, C, T, cells, kvg)),
        out_shape=jax.ShapeDtypeStruct((D * tokens, C * qcols), bf16),
        in_specs=[pl.BlockSpec(memory_space=pltpu.VMEM)] * 5,
        out_specs=pl.BlockSpec(memory_space=pltpu.VMEM),
        scratch_shapes=[
            pltpu.VMEM((S * depth, width), bf16),
            pltpu.VMEM((channels, DIM), bf16),
            pltpu.VMEM((16, DIM), bf16),
            pltpu.VMEM((C, D * tokens, channels), bf16),
            pltpu.VMEM((C, D * tokens, DIM), bf16),
            pltpu.VMEM((C, D * tokens, HEAD), f32),
            pltpu.VMEM((C, D * tokens, qcols), bf16),
            dma((C, T)),
            dma((C, T)),
            dma((C, T, D)),
            dma((C, T, D)),
            dma((C, D)),
            dma((C, D)),
            dma((D,)),
            dma((D,)),
            dma((C,)),
            dma((C,)),
            dma((4,)),
        ],
        compiler_params=pltpu.CompilerParams(
            collective_id=0, has_side_effects=True, vmem_limit_bytes=60 * 1024 * 1024
        ),
    )(pack, w_in, aux, latent, pick)
    return out.reshape(D, frames, height, breadth, -1)


def solution(mesh):
    placed = (
        P("dp", None, "seq", None, None),
        P("dp", None, "seq", None),
        P(),
        P(),
        P(),
        P(),
        P(),
        P("seq", "dp"),
        P(None, "dp"),
        P("dp"),
        P("seq", "dp"),
        P("seq", None, "dp"),
        P(),
    )
    return jax.shard_map(
        body,
        mesh=mesh,
        in_specs=placed,
        out_specs=P(None, None, "seq", None, "dp"),
        check_vma=False,
    )
```

```python
import functools
import math

import jax
import jax.numpy as jnp
from jax import lax
from jax.experimental import pallas as pl
from jax.experimental.pallas import tpu as pltpu
from jax.sharding import PartitionSpec as P

DIM = 5120
HEAD = 128
Q_HEADS = 40
KV_HEADS = 8
MESH = pl.DeviceIdType.MESH


def gelu(z):
    return 0.5 * z * (1.0 + jnp.tanh(0.7978845608028654 * (z + 0.044715 * (z * z * z))))


def flipped(t, mask, bits):
    for bit in bits:
        if mask & bit:
            t = t + bit - 2 * bit * ((t // bit) % 2)
    return t


def window_kernel(
    sizes,
    pack_ref,
    in_ref,
    aux_ref,
    start_ref,
    taps_ref,
    gains_ref,
    point_ref,
    pick_ref,
    out_ref,
    w_all,
    in_all,
    aux_all,
    lat_all,
    embeds,
    squares,
    mixed,
    halos,
    middle,
    conv,
    latent_ref,
    h_send,
    h_recv,
    w_send,
    w_recv,
    i_send,
    i_recv,
    l_send,
    l_recv,
    a_send,
    a_recv,
    o_send,
    o_recv,
    own_sem,
):
    D, C, T, cells, kvg = sizes
    d = lax.axis_index("dp")
    seq = lax.axis_index("seq")
    c = seq // T
    t = seq % T
    bits = []
    bit = T // 2
    while bit:
        bits.append(bit)
        bit //= 2
    depth = pack_ref.shape[1]
    in_rows, in_cols = in_ref.shape
    tokens = latent_ref.shape[0]
    group = Q_HEADS // KV_HEADS
    qcols = kvg * group * HEAD

    def to_c(shift):
        return (d, ((c + shift) % C) * T + t)

    def to_t(bit):
        return (d, c * T + flipped(t, bit, bits))

    def to_d(shift):
        return ((d + shift) % D, seq)

    peers = [to_c(s) for s in range(1, C)] + [to_t(b) for b in bits] + [to_d(s) for s in range(1, D)]
    S = C * T
    above, below = (d, (seq + S - 1) % S), (d, (seq + 1) % S)
    peers += [above, below]
    barrier = pltpu.get_barrier_semaphore()
    for peer in peers:
        pl.semaphore_signal(barrier, inc=1, device_id=peer, device_id_type=MESH)
    pl.semaphore_wait(barrier, len(peers))

    sends = []

    def push(src, dst, send_sem, recv_sem, peer):
        copy = pltpu.make_async_remote_copy(
            src_ref=src,
            dst_ref=dst,
            send_sem=send_sem,
            recv_sem=recv_sem,
            device_id=peer,
            device_id_type=MESH,
        )
        copy.start()
        sends.append(copy)

    def arrived(ref, sem):
        pltpu.make_async_copy(ref, ref, sem).wait()

    def w_slot(s, m):
        origin = ((c + C - s) % C) * T + flipped(t, m, bits)
        return w_all.at[pl.ds(pl.multiple_of(origin * depth, depth), depth)]

    def i_slot(s, m, e):
        origin = ((c + C - s) % C) * T + flipped(t, m, bits)
        column = ((d + D - e) % D) * in_cols
        return in_all.at[
            pl.ds(pl.multiple_of(origin * in_rows, in_rows), in_rows),
            pl.ds(pl.multiple_of(column, HEAD), in_cols),
        ]

    def l_slot(s, e):
        row = ((d + D - e) % D) * tokens
        return lat_all.at[(c + C - s) % C, pl.ds(pl.multiple_of(row, tokens), tokens)]

    def a_slot(e):
        column = ((d + D - e) % D) * in_cols
        return aux_all.at[:, pl.ds(pl.multiple_of(column, HEAD), in_cols)]

    def w_forward(s, m, src):
        low = -1
        for b in bits:
            if m & b:
                low = bits.index(b)
        for index in range(low + 1, len(bits)):
            b = bits[index]
            push(src, w_slot(s, m), w_send.at[s, m | b], w_recv.at[s, m | b], to_t(b))

    early, last = bits[:-1], bits[-1]

    def i_forward(s, m, e, src):
        low = -1
        for b in early:
            if m & b:
                low = bits.index(b)
        if e == 0:
            for index in range(low + 1, len(early)):
                b = early[index]
                push(src, i_slot(s, m, e), i_send.at[s, m | b, e], i_recv.at[s, m | b, e], to_t(b))
            for shift in range(1, D):
                push(src, i_slot(s, m, e), i_send.at[s, m, shift], i_recv.at[s, m, shift], to_d(shift))
        push(src, i_slot(s, m, e), i_send.at[s, m | last, e], i_recv.at[s, m | last, e], to_t(last))

    def l_forward(s, src):
        for e in range(1, D):
            push(src, l_slot(s, 0), l_send.at[s, e], l_recv.at[s, e], to_d(e))

    own = [
        pltpu.make_async_copy(pack_ref.at[c], w_slot(0, 0), own_sem.at[0]),
        pltpu.make_async_copy(in_ref, i_slot(0, 0, 0), own_sem.at[1]),
        pltpu.make_async_copy(aux_ref, a_slot(0), own_sem.at[3]),
    ]
    for copy in own:
        copy.start()
    height, breadth, frames, channels = start_ref.shape

    def share_rows(l, source):
        push(source.at[height - 1], halos.at[l, 0], h_send.at[l, 0], h_recv.at[l, 0], below)
        push(source.at[0], halos.at[l, 1], h_send.at[l, 1], h_recv.at[l, 1], above)

    share_rows(0, start_ref)
    for shift in range(1, D):
        push(aux_ref, a_slot(0), a_send.at[shift], a_recv.at[shift], to_d(shift))
    for shift in range(1, C):
        push(in_ref, i_slot(0, 0, 0), i_send.at[shift, 0, 0], i_recv.at[shift, 0, 0], to_c(shift))
    i_forward(0, 0, 0, in_ref)
    for shift in range(1, C):
        push(
            pack_ref.at[(c + shift) % C],
            w_slot(0, 0),
            w_send.at[shift, 0],
            w_recv.at[shift, 0],
            to_c(shift),
        )
    w_forward(0, 0, pack_ref.at[c])

    def i_event(s, m, e):
        arrived(i_slot(s, m, e), i_recv.at[s, m, e])
        if not m & last:
            i_forward(s, m, e, i_slot(s, m, e))

    def w_event(s, m):
        arrived(w_slot(s, m), w_recv.at[s, m])
        w_forward(s, m, w_slot(s, m))

    def l_event(s, e):
        arrived(l_slot(s, e), l_recv.at[s, e])
        if e == 0:
            l_forward(s, l_slot(s, e))

    lanes = 256

    def encode(l, source):
        arrived(halos.at[l, 0], h_recv.at[l, 0])
        arrived(halos.at[l, 1], h_recv.at[l, 1])
        frame_ids = lax.broadcasted_iota(jnp.int32, (frames, lanes), 0)

        def lane_step(j, carry):
            cols = pl.ds(pl.multiple_of(j * lanes, lanes), lanes)
            taps = taps_ref[l, :, cols].astype(jnp.float32)

            def patch(r, w):
                if r < 0:
                    return jnp.where(seq > 0, halos[l, 0, w, :, cols].astype(jnp.float32), 0.0)
                if r == height:
                    return jnp.where(seq < S - 1, halos[l, 1, w, :, cols].astype(jnp.float32), 0.0)
                return source[r, w, :, cols].astype(jnp.float32)

            for r in range(height):
                for w in range(breadth):
                    sums = [None] * 3
                    for b in range(3):
                        for k in range(3):
                            if not 0 <= w + k - 1 < breadth:
                                continue
                            value = patch(r + b - 1, w + k - 1)
                            for a in range(3):
                                tap = 9 * a + 3 * b + k
                                term = value * taps[tap : tap + 1]
                                sums[a] = term if sums[a] is None else sums[a] + term
                    total = sums[2]
                    for a in range(2):
                        moved = pltpu.roll(sums[a], 2 - a, 0)
                        total = total + jnp.where(frame_ids >= 2 - a, moved, 0.0)
                    base = (r * breadth + w) * frames
                    conv[base : base + frames, cols] = total
            return carry

        lax.fori_loop(0, channels // lanes, lane_step, 0)
        summed = conv[...]
        factor = lax.rsqrt(jnp.mean(summed * summed, axis=-1, keepdims=True) + 1e-05)
        gain = gains_ref[l].astype(jnp.float32)
        normed = (summed * factor * gain[None]).astype(jnp.bfloat16)
        projected = jnp.dot(normed, point_ref[l], preferred_element_type=jnp.float32)
        change = gelu(projected)
        for r in range(height):
            for w in range(breadth):
                base = (r * breadth + w) * frames
                value = source[r, w].astype(jnp.float32) + change[base : base + frames]
                value = value.astype(jnp.bfloat16)
                if l + 1 < point_ref.shape[0]:
                    middle[l, r, w] = value
                else:
                    latent_ref[base : base + frames] = value

    source = start_ref
    for l in range(point_ref.shape[0]):
        encode(l, source)
        if l + 1 < point_ref.shape[0]:
            source = middle.at[l]
            share_rows(l + 1, source)
            for s in range(1, C):
                i_event(s, 0, 0)
    for shift in range(1, C):
        push(latent_ref, l_slot(0, 0), l_send.at[shift, 0], l_recv.at[shift, 0], to_c(shift))
    l_forward(0, latent_ref)
    latent_copy = pltpu.make_async_copy(latent_ref, l_slot(0, 0), own_sem.at[2])
    latent_copy.start()
    own.append(latent_copy)

    order_w = sorted(
        ((m.bit_count(), s, m) for s in range(C) for m in range(T) if s or m),
        key=lambda item: (item[0] + item[1], item[0]),
    )
    w_todo = [(s, m) for _, s, m in order_w]
    for m in sorted((m for m in range(1, T) if not m & last), key=lambda m: m.bit_count()):
        for s in range(C):
            i_event(s, m, 0)
    for s in range(1, C):
        l_event(s, 0)
    for e in range(1, D):
        arrived(a_slot(e), a_recv.at[e])
        for m in range(T):
            if not m & last:
                for s in range(C):
                    i_event(s, m, e)
    for s, m in list(w_todo):
        if m == 0:
            w_event(s, m)
            w_todo.remove((s, m))
    for m in range(T):
        if m & last:
            for e in range(D):
                for s in range(C):
                    i_event(s, m, e)
    for e in range(1, D):
        for s in range(C):
            l_event(s, e)
    for copy in own:
        copy.wait()

    chunk = 512
    rows = D * tokens

    def embed_block(shift):
        where = (c + shift) % C
        squares[where] = jnp.zeros((rows, HEAD), jnp.float32)

        def step(j, carry):
            cols = pl.ds(pl.multiple_of(j * chunk, chunk), chunk)
            z = jnp.dot(lat_all[where], in_all[:, cols], preferred_element_type=jnp.float32)
            z = z + jnp.dot(pick_ref[...], aux_all[:, cols], preferred_element_type=jnp.float32)
            g = gelu(z)
            gain = aux_all[:, cols].astype(jnp.float32)[8:9]
            embeds[where, :, cols] = (g * gain).astype(jnp.bfloat16)
            square = g * g
            part = square[:, :HEAD]
            for k in range(1, chunk // HEAD):
                part = part + square[:, k * HEAD : (k + 1) * HEAD]
            squares[where] += part
            return carry

        lax.fori_loop(0, embeds.shape[2] // chunk, step, 0)

    per = -(-len(w_todo) // C)
    for shift in range(C):
        embed_block(shift)
        for s, m in w_todo[shift * per : (shift + 1) * per]:
            w_event(s, m)

    row_ids = lax.broadcasted_iota(jnp.int32, (tokens, tokens), 0)
    col_ids = lax.broadcasted_iota(jnp.int32, (tokens, tokens), 1)
    seen = (row_ids // frames == col_ids // frames) & (row_ids >= col_ids)

    def unit(x):
        return x * lax.rsqrt(jnp.mean(x * x, axis=-1, keepdims=True) + 1e-06)

    def mix_block(where):
        total = jnp.dot(embeds[where], w_all[...], preferred_element_type=jnp.float32)
        mean = jnp.sum(squares[where], axis=-1, keepdims=True) / DIM
        total = total * lax.rsqrt(mean + 1e-05)
        for kv in range(kvg):
            at = qcols + kv * HEAD
            key = unit(total[:, at : at + HEAD]).astype(jnp.bfloat16)
            at = qcols + (kvg + kv) * HEAD
            value = total[:, at : at + HEAD].astype(jnp.bfloat16)
            for h in range(kv * group, (kv + 1) * group):
                query = unit(total[:, h * HEAD : (h + 1) * HEAD]) * HEAD**-0.5
                query = query.astype(jnp.bfloat16)
                for clip in range(D):
                    span = slice(clip * tokens, (clip + 1) * tokens)
                    score = lax.dot_general(
                        query[span],
                        key[span],
                        (((1,), (1,)), ((), ())),
                        preferred_element_type=jnp.float32,
                    )
                    raised = jnp.where(seen, jnp.exp(score), 0.0)
                    shares = raised / jnp.sum(raised, axis=-1, keepdims=True)
                    result = jnp.dot(
                        shares.astype(jnp.bfloat16), value[span], preferred_element_type=jnp.float32
                    )
                    mixed[where, span, h * HEAD : (h + 1) * HEAD] = result.astype(jnp.bfloat16)

    mine = pl.ds(pl.multiple_of(c * qcols, HEAD), qcols)

    def send_of(shift):
        where = (c + shift) % C
        return pltpu.make_async_remote_copy(
            src_ref=mixed.at[where],
            dst_ref=out_ref.at[:, mine],
            send_sem=o_send.at[shift],
            recv_sem=o_recv.at[shift],
            device_id=(d, where * T + t),
            device_id_type=MESH,
        )

    def mix_step(index, carry):
        shift = index + 1
        mix_block((c + shift) % C)
        send_of(shift).start()
        return carry

    lax.fori_loop(0, C - 1, mix_step, 0)
    mix_block(c)
    keep = pltpu.make_async_copy(mixed.at[c], out_ref.at[:, mine], own_sem.at[0])
    keep.start()
    for shift in range(1, C):
        send_of(shift).wait_send()
        column = ((c + C - shift) % C) * qcols
        arrived(out_ref.at[:, pl.ds(pl.multiple_of(column, HEAD), qcols)], o_recv.at[shift])
    keep.wait()
    for copy in sends:
        copy.wait_send()


def body(
    tiles,
    patch_index,
    pos_table,
    depth_kernel,
    enc_gain,
    point_weight,
    action_ids,
    w_in,
    action_table,
    dyn_gain,
    w_query,
    w_keyval,
    seq_order,
):
    clip_local, frames, height, breadth, channels = tiles.shape
    positions = pos_table.shape[0]
    blocks = depth_kernel.shape[0]
    D, S = lax.axis_size("dp"), lax.axis_size("seq")
    kv_local = w_keyval.shape[2] // HEAD
    C = math.gcd(kv_local, S)
    T = S // C
    assert T & (T - 1) == 0 and T > 1 and clip_local == 1
    kvg = kv_local // C
    group = Q_HEADS // KV_HEADS
    depth = w_query.shape[0]
    frames_first = (0, 3, 1, 2, 4)

    flat_index = patch_index.reshape(-1)
    position_pick = (flat_index[:, None] == jnp.arange(positions, dtype=jnp.int32)[None, :]).astype(
        jnp.bfloat16
    )
    placed = jnp.dot(position_pick, pos_table, preferred_element_type=jnp.float32).reshape(
        tiles.shape
    )
    hidden = (tiles.astype(jnp.float32) + placed).astype(jnp.bfloat16)
    start = hidden[0].transpose(1, 2, 0, 3)

    cells = height * breadth
    tokens = frames * cells
    pack = jnp.concatenate(
        [
            w_query.reshape(depth, C, -1).transpose(1, 0, 2),
            w_keyval.reshape(depth, 2, C, -1).transpose(2, 0, 1, 3).reshape(C, depth, -1),
        ],
        axis=2,
    )
    actions = action_table.shape[0]
    assert actions == 8
    aux = jnp.concatenate(
        [action_table, dyn_gain[None], jnp.zeros((7, action_table.shape[1]), jnp.bfloat16)], axis=0
    )
    pick = (
        jnp.tile(action_ids[:, None, :], (1, cells, 1)).reshape(-1)[:, None] == jnp.arange(16, dtype=jnp.int32)[None]
    ).astype(jnp.bfloat16)
    width = pack.shape[2]
    qcols = kvg * group * HEAD
    bf16, f32 = jnp.bfloat16, jnp.float32
    dma = pltpu.SemaphoreType.DMA
    out = pl.pallas_call(
        functools.partial(window_kernel, (D, C, T, cells, kvg)),
        out_shape=jax.ShapeDtypeStruct((D * tokens, C * qcols), bf16),
        in_specs=[pl.BlockSpec(memory_space=pltpu.VMEM)] * 8,
        out_specs=pl.BlockSpec(memory_space=pltpu.VMEM),
        scratch_shapes=[
            pltpu.VMEM((S * depth, width), bf16),
            pltpu.VMEM((channels, DIM), bf16),
            pltpu.VMEM((16, DIM), bf16),
            pltpu.VMEM((C, D * tokens, channels), bf16),
            pltpu.VMEM((C, D * tokens, DIM), bf16),
            pltpu.VMEM((C, D * tokens, HEAD), f32),
            pltpu.VMEM((C, D * tokens, qcols), bf16),
            pltpu.VMEM((blocks, 2, breadth, frames, channels), bf16),
            pltpu.VMEM((max(blocks - 1, 1), height, breadth, frames, channels), bf16),
            pltpu.VMEM((tokens, channels), f32),
            pltpu.VMEM((tokens, channels), bf16),
            dma((blocks, 2)),
            dma((blocks, 2)),
            dma((C, T)),
            dma((C, T)),
            dma((C, T, D)),
            dma((C, T, D)),
            dma((C, D)),
            dma((C, D)),
            dma((D,)),
            dma((D,)),
            dma((C,)),
            dma((C,)),
            dma((4,)),
        ],
        compiler_params=pltpu.CompilerParams(
            collective_id=0, has_side_effects=True, vmem_limit_bytes=60 * 1024 * 1024
        ),
    )(pack, w_in, aux, start, depth_kernel, enc_gain, point_weight, pick)
    out = out.reshape(D, height, breadth, frames, -1).transpose(frames_first)
    return jnp.take(out, seq_order, axis=3)


def solution(mesh):
    placed = (
        P("dp", None, "seq", None, None),
        P("dp", None, "seq", None),
        P(),
        P(),
        P(),
        P(),
        P(),
        P("seq", "dp"),
        P(None, "dp"),
        P("dp"),
        P("seq", "dp"),
        P("seq", None, "dp"),
        P(),
    )
    return jax.shard_map(
        body,
        mesh=mesh,
        in_specs=placed,
        out_specs=P(None, None, "seq", None, "dp"),
        check_vma=False,
    )
```
